32 devices in a mesh: grp: 2 (over core), shard: 16 (over z, y, x).
Axes of the slice: x: 2, y: 2, z: 4, core: 2. Of those that a mesh axis runs over, the one named last changes fastest.
Arguments:
- blocks: float32 [2048, 128, 128], P(('grp', 'shard')), may hold values from -0.1875 to 0.1875
- block_row: int32 [2048], P(('grp', 'shard')), may hold values from 0 to 511, as said below
- block_owner: int32 [2048, 1], P(('grp', 'shard')), may hold values from 0 to 15; in each aligned block of 64 rows (0 to 63, 64 to 127, ...) at most 8 rows name the same one
- block_col: int32 [2048], P(('grp', 'shard')), may hold values from 0 to 15
- right_side: float32 [65536, 8], P(('grp', 'shard')), may hold values from -6 to 6
Outputs:
- solution: float32 [32768, 8], P('shard')
- left_vector: float32 [65536, 8], P(('grp', 'shard'))
- rel_residual: float32 [8], replicated
The draws below stay inside these ranges and needn't reach their ends.
Inputs may be any that keep to these rules, and one draw needn't show every extreme that they name: `block_row`: block k lies in a row block of the device that holds it: between (k // 64) * 16 and (k // 64) * 16 + 15. `block_owner`: among the 64 blocks of one device, each owner is named at most 8 times, and in every draw some device names some owner exactly 8 times. `block_col`: a column block index among the 16 of the owner.
All inputs are finite; a program needn't handle non-finite values.
Results may differ from the reference program's by a relative error of at most 0.00024.
Values sent between devices are 32-bit elements; how exact they have to be, the bound alone decides.
A program may use at most 64 MiB of HBM per device.

```python
import math
import jax
import jax.numpy as jnp
import numpy as np
from jax import lax

BS = 128
RHS = 8
ITERS = 4
BLK_DEV = 64
ROWS_DEV = 16
COLS_OWN = 16
CAP = 8
TOTAL_BLK = 2048
RB = 512
CB = 256
BLK_COL = 8
N_SHARD = 16


def draw_block_row(key, part):
    local = jax.random.randint(key, (TOTAL_BLK,), 0, ROWS_DEV, dtype=jnp.int32)
    holder = jnp.arange(TOTAL_BLK, dtype=jnp.int32) // BLK_DEV
    return (holder * ROWS_DEV + local).astype(jnp.int32)


def touch_ends(result, rng, smallest, top_value):
    index_at = [jax.random.randint(jax.random.fold_in(rng, axis), (), 0, length) for axis, length in enumerate(result.shape)]
    widest = result.shape.index(max(result.shape))
    neighbour = index_at[:widest] + [(index_at[widest] + 1) % result.shape[widest]] + index_at[widest + 1:]
    return result.at[tuple(index_at)].set(smallest).at[tuple(neighbour)].set(top_value)


def levels(key, shape, cuts, least, high):
    factor_of, own = 1.0, jax.random.fold_in(key, 6)
    for dim, parts in cuts:
        steps = jnp.exp(jax.random.uniform(jax.random.fold_in(own, dim), (parts,), jnp.float32, least / len(cuts), high / len(cuts)))
        factor_of = factor_of * jnp.repeat(steps, shape[dim] // parts).reshape([-1 if axis == dim else 1 for axis in range(len(shape))])
    return factor_of


def shared_out(own_key, own, number, rows, number_of, top, bound, lean):
    order = jax.random.permutation(own_key, number_of)
    crowded, ordinary = portions_of(number_of, rows * top, bound, lean, True), portions_of(number_of, rows * top, bound, lean, False)
    places = jnp.arange(number_of)

    def named(sizes, rotation):
        used = int((sizes > 0).sum())
        fixed = max(1, used // 4)
        passed = fixed + (places - fixed + rotation * (used - fixed)) % max(1, number_of - fixed)
        return jnp.zeros((number_of,), jnp.int32).at[order[jnp.where(places < fixed, places, passed)]].set(jnp.asarray(sizes, jnp.int32))

    sizes = jnp.where(number % 4 == 0, named(crowded, number // 4), named(ordinary, number - number // 4 - 1))
    mixed = jax.random.permutation(jax.random.fold_in(own, 3), number_of)
    giver, receiver = mixed[0:number_of // 2 * 2:2], mixed[1:number_of // 2 * 2:2]
    room = jnp.minimum(sizes[giver] - 1, bound - sizes[receiver]) // 2
    room = jnp.where((giver == order[0]) | (receiver == order[0]) | (sizes[receiver] == 0), 0, jnp.maximum(room, 0))
    passed = jax.random.randint(jax.random.fold_in(own, 4), (number_of // 2,), 0, 1 << 20) % (room + 1)
    sizes = sizes.at[giver].add(-passed).at[receiver].add(passed)
    labels = jnp.searchsorted(jnp.cumsum(sizes), jnp.arange(rows * top), side="right").astype(jnp.int32)
    grid = labels.reshape(top, rows).T
    grid = grid[jax.random.permutation(jax.random.fold_in(own, 1), rows)]
    rotation = jax.random.randint(jax.random.fold_in(own, 2), (rows, 1), 0, top)
    return jnp.take_along_axis(grid, (jnp.arange(top)[None, :] + rotation) % top, axis=1)


def portions_of(number_of, total, reach, lean, full):
    weights = [(1 << 20) // math.isqrt(standing ** lean) + 1 for standing in range(1, number_of + 1)]
    largest = reach if full else min(reach, max(-(-total // number_of), total * weights[0] // sum(weights)))
    least = 1 if total - largest >= number_of - 1 else 0
    holding, surplus = [largest] + [least] * (number_of - 1), total - largest - least * (number_of - 1)
    while surplus > 0:
        free = [i for i in range(1, number_of) if holding[i] < largest] or [i for i in range(1, number_of) if holding[i] < reach]
        pool, left = sum([weights[i] for i in free]), surplus
        for i in free:
            more = min(reach - holding[i], max(1, left * weights[i] // pool), surplus)
            holding[i] = holding[i] + more
            surplus = surplus - more
    return np.array(holding)


def normal_values(rng, dims, scale, most, cuts=(), kind=jnp.bfloat16):
    drawn = scale * jax.random.normal(rng, dims, jnp.float32)
    if cuts:
        drawn = drawn * levels(rng, dims, cuts, -0.22, 0.18)
    return jnp.clip(drawn, -most, most).astype(kind)


def setup_inputs(seed: int = 0) -> dict:
    keys = jax.random.split(jax.random.key(seed), 6)
    blocks = normal_values(keys[0], (TOTAL_BLK, BS, BS), (BS * BLK_COL) ** -0.5, 0.1875, ((0, 32),), jnp.float32)
    block_row = draw_block_row(jax.random.fold_in(keys[5], 71), 0)
    block_owner_keys = jax.random.split(jax.random.fold_in(keys[2], 1), TOTAL_BLK // BLK_DEV)
    block_owner_turns = jax.random.permutation(jax.random.fold_in(keys[2], 3), TOTAL_BLK // BLK_DEV)
    block_owner = jax.vmap(lambda own, number: shared_out(jax.random.fold_in(keys[2], 2), own, number, BLK_DEV, N_SHARD, 1, CAP, 2))(block_owner_keys, block_owner_turns).reshape((TOTAL_BLK, 1))
    block_col = touch_ends(jax.random.randint(keys[3], (TOTAL_BLK,), 0, COLS_OWN), jax.random.fold_in(keys[3], 1), 0, COLS_OWN - 1).astype(jnp.int32)
    right_side = normal_values(keys[4], (RB * BS, RHS), 1.0, 6.0, ((0, 32),), jnp.float32)
    return dict(blocks=blocks, block_row=block_row, block_owner=block_owner, block_col=block_col, right_side=right_side)


PRECISE = lax.Precision.HIGHEST

def forward(blocks, row_index, col_index, vector):
    pieces = vector.reshape(CB, BS, RHS)[col_index]
    product = jnp.einsum('kij,kjr->kir', blocks, pieces, precision=PRECISE)
    summed = jax.ops.segment_sum(product, row_index, num_segments=RB)
    return summed.reshape(RB * BS, RHS)

def adjoint(blocks, row_index, col_index, vector):
    pieces = vector.reshape(RB, BS, RHS)[row_index]
    product = jnp.einsum('kij,kir->kjr', blocks, pieces, precision=PRECISE)
    summed = jax.ops.segment_sum(product, col_index, num_segments=CB)
    return summed.reshape(CB * BS, RHS)

def column_norm(values):
    return jnp.sqrt(lax.optimization_barrier(jnp.sum(values * values, axis=0)))

def rotate(state, norm_left, norm_right, right_vec):
    solution, search, diag_bar, residual_norm = state
    radius = jnp.sqrt(diag_bar * diag_bar + norm_left * norm_left)
    cosine = diag_bar / radius
    sine_term = norm_left / radius
    coupling = sine_term * norm_right
    step_size = cosine * residual_norm
    solution = solution + step_size / radius * search
    search = right_vec - coupling / radius * search
    return (solution, search, -cosine * norm_right, sine_term * residual_norm)

def reference(blocks, block_row, block_owner, block_col, right_side):
    col_index = (block_owner[:, 0] * COLS_OWN + block_col).astype(jnp.int32)
    row_index = block_row.astype(jnp.int32)
    norm_start = column_norm(right_side)
    left_vec = right_side / norm_start
    right_vec = adjoint(blocks, row_index, col_index, left_vec)
    norm_right = column_norm(right_vec)
    right_vec = right_vec / norm_right
    state = (jnp.zeros_like(right_vec), right_vec, norm_right, norm_start)
    for repeat in range(ITERS):
        left_raw = forward(blocks, row_index, col_index, right_vec) - norm_right * left_vec
        norm_left = column_norm(left_raw)
        left_vec = left_raw / norm_left
        right_raw = adjoint(blocks, row_index, col_index, left_vec) - norm_left * right_vec
        norm_right = column_norm(right_raw)
        right_vec = right_raw / norm_right
        state = rotate(state, norm_left, norm_right, right_vec)
    return (state[0], left_vec, state[3] / norm_start)
```

```python
import functools

import jax
import jax.numpy as jnp
from jax import lax
from jax.experimental import pallas as pl
from jax.experimental.pallas import tpu as pltpu
from jax.sharding import PartitionSpec as P

ITERS = 4
COLS_OWN = 16
HALF = COLS_OWN // 2
PLANE = 4
LOADS = 8
MESH = pl.DeviceIdType.MESH
F32 = jnp.float32
BF16 = jnp.bfloat16


def split(value):
    high = value.astype(BF16).astype(F32)
    return high, value - high


def total(tile):
    return jnp.broadcast_to(jnp.sum(tile, axis=-1, keepdims=True), tile.shape)


def kernel(
    shards, count, rows,
    owner_ref, col_ref, row_ref, code_ref, blocks_ref, right_ref,
    sol_ref, left_out, rel_ref,
    raw, pair, scatter, gather_rows, prod, left, unit, image,
    full, part, cross, from_a, from_b, relay, from_z, to_z, norms, norms_in,
    own, search, bidiag,
    load_sem, x_send, x_recv, a_send, a_recv, b_send, b_recv, c_send, c_recv,
    z_send, z_recv, p_send, p_recv, g_send, g_recv, n_send, n_recv,
):
    line = shards // PLANE
    grp = lax.axis_index("grp")
    me = lax.axis_index("shard")
    high, low = me // PLANE, me % PLANE

    def flip(d):
        bit0 = low % 2
        bit1 = low // 2
        if d & 1:
            bit0 = 1 - bit0
        if d & 2:
            bit1 = 1 - bit1
        return bit1 * 2 + bit0

    lows = [flip(d) for d in range(PLANE)]
    ahead = [lax.rem(high + e, line) for e in range(line)]
    behind = [lax.rem(high + line - e, line) for e in range(line)]
    partner = (1 - grp, me)
    plane = {d: (grp, high * PLANE + lows[d]) for d in (1, 2)}
    along = {e: (grp, ahead[e] * PLANE + low) for e in range(1, line)}

    def remote(src, dst, send, recv, device):
        return pltpu.make_async_remote_copy(
            src_ref=src, dst_ref=dst, send_sem=send, recv_sem=recv,
            device_id=device, device_id_type=MESH,
        )

    per_load = count // LOADS
    loads = [
        pltpu.make_async_copy(
            blocks_ref.at[pl.ds(i * per_load, per_load)],
            raw.at[pl.ds(i * per_load, per_load)],
            load_sem.at[i],
        )
        for i in range(LOADS)
    ]
    for copy in loads:
        copy.start()

    barrier = pltpu.get_barrier_semaphore()
    greeted = [partner, plane[1], plane[2]] + [along[e] for e in range(1, line)]
    for device in greeted:
        pl.semaphore_signal(barrier, inc=1, device_id=device, device_id_type=MESH)

    squares = jnp.zeros((8, 128), F32)
    for r in range(rows):
        tile = right_ref[:, r * 128:(r + 1) * 128]
        left[r] = tile
        squares = squares + tile * tile
    norms[0] = squares

    codes = code_ref[0:1, :]
    row_codes = code_ref[1:2, :]
    ids = lax.broadcasted_iota(jnp.int32, (HALF * 8, count * 8), 0)

    def build(q, carry):
        scatter[q] = jnp.where(ids + q * (HALF * 8) == codes, 1.0, 0.0).astype(BF16)
        return carry

    lax.fori_loop(0, 2 * shards, build, 0)
    row_ids = lax.broadcasted_iota(jnp.int32, (rows * 8, count * 8), 0)
    gather_rows[...] = jnp.where(row_ids == row_codes, 1.0, 0.0).astype(BF16)

    for i, copy in enumerate(loads):
        copy.wait()

        def narrow(k, carry):
            block = raw[k]
            upper = block.astype(BF16)
            pair[k, :, 0:128] = upper
            pair[k, :, 128:256] = (block - upper.astype(F32)).astype(BF16)
            return carry

        lax.fori_loop(i * per_load, (i + 1) * per_load, narrow, 0, unroll=2)

    for j in range(COLS_OWN):
        own[j] = jnp.zeros((8, 128), F32)
        search[j] = jnp.zeros((8, 128), F32)
        sol_ref[:, j * 128:(j + 1) * 128] = jnp.zeros((8, 128), F32)

    pl.semaphore_wait(barrier, len(greeted))

    def both(tile):
        upper, lower = split(tile)
        return jnp.concatenate([upper, lower], axis=0).astype(BF16)

    def store_products(step, tiles):
        merged = jnp.concatenate(tiles, axis=0)
        upper, lower = split(merged)
        start = pl.multiple_of(step * 8 * len(tiles), 16)
        prod[pl.ds(start, 8 * len(tiles)), 0:128] = upper.astype(BF16)
        prod[pl.ds(start, 8 * len(tiles)), 128:256] = lower.astype(BF16)

    def adjoint(step, carry):
        tiles = []
        for i in range(4):
            k = step * 4 + i
            out = jnp.dot(both(left[row_ref[k] % rows]), pair[k], preferred_element_type=F32)
            out = out[:, 0:128] + out[:, 128:256]
            tiles.append(out[0:8] + out[8:16])
        store_products(step, tiles)
        return carry

    def forward(step, carry):
        tiles = []
        for i in range(4):
            k = step * 4 + i
            col = col_ref[k]
            tile = full[(col // HALF) * shards + owner_ref[k], col % HALF]
            lhs = both(tile)
            lhs = jnp.concatenate([lhs, lhs], axis=1)
            out = lax.dot_general(
                lhs, pair[k], (((1,), (1,)), ((), ())), preferred_element_type=F32
            )
            tiles.append(out[0:8] + out[8:16])
        store_products(step, tiles)
        return carry

    def columns_of(half):
        for c in range(shards // 16):
            base = half * shards + c * 16
            lhs = scatter[pl.ds(base, 16)].reshape(16 * HALF * 8, count * 8)
            out = jnp.dot(lhs, prod[...], preferred_element_type=F32)
            out = out[:, 0:128] + out[:, 128:256]
            part[pl.ds(base, 16), 0:HALF] = out.reshape(16, HALF, 8, 128)
            part[pl.ds(base, 16), HALF] = jnp.broadcast_to(norms[0][None], (16, 8, 128))

    def reduce_scatter():
        sends = []
        columns_of(1 - grp)
        order = [e for e in range(1, line)] + [0]
        exchange = {}
        for e in order:
            first = ahead[e] * PLANE
            exchange[e] = remote(
                part.at[pl.ds((1 - grp) * shards + first, PLANE)],
                cross.at[pl.ds(first, PLANE)],
                x_send.at[e], x_recv.at[e], partner,
            )
            exchange[e].start()
        columns_of(grp)
        stage_a = {}
        for e in order:
            exchange[e].wait_recv()
            first = ahead[e] * PLANE
            cross[pl.ds(first, PLANE)] = (
                cross[pl.ds(first, PLANE)] + part[pl.ds(grp * shards + first, PLANE)]
            )
            a = 1 if e % 2 == 0 else 2
            for i, d in enumerate((3, a)):
                copy = remote(
                    cross.at[first + lows[d]], from_a.at[e, i],
                    a_send.at[e, i], a_recv.at[e, i], plane[a],
                )
                copy.start()
                stage_a[e, i] = copy
        stage_b = {}
        for e in order:
            first = ahead[e] * PLANE
            b = 2 if e % 2 == 0 else 1
            stage_a[e, 0].wait_recv()
            relay[e] = cross[first + lows[b]] + from_a[e, 0]
            stage_b[e] = remote(relay.at[e], from_b.at[e], b_send.at[e], b_recv.at[e], plane[b])
            stage_b[e].start()
        stage_c = {}
        for e in order:
            first = ahead[e] * PLANE
            stage_a[e, 1].wait_recv()
            mine = cross[first + low] + from_a[e, 1]
            stage_b[e].wait_recv()
            to_z[e] = mine + from_b[e]
            if e:
                stage_c[e] = remote(
                    to_z.at[e], from_z.at[e - 1], c_send.at[e - 1], c_recv.at[e - 1], along[e]
                )
                stage_c[e].start()
        for e in range(1, line):
            stage_c[e].wait_recv()
        summed = to_z[0]
        for e in range(1, line):
            summed = summed + from_z[e - 1]
        for copies in (exchange, stage_a, stage_b, stage_c):
            for copy in copies.values():
                copy.wait_send()
        return summed

    def slot(e, d):
        return grp * shards + behind[e] * PLANE + lows[d]

    def all_gather():
        sends = []

        def piece(e, d, send, recv, device):
            place = full.at[slot(e, d)]
            return remote(place, place, send, recv, device)

        for e in range(1, line):
            copy = piece(0, 0, z_send.at[e - 1], z_recv.at[e - 1], along[e])
            copy.start()
            sends.append(copy)

        def spread(e):
            for d in (1, 2):
                copy = piece(e, 0, p_send.at[d - 1, e], p_recv.at[d - 1, e], plane[d])
                copy.start()
                sends.append(copy)
            hand(e, 0)

        def hand(e, d):
            copy = piece(e, d, g_send.at[d, e], g_recv.at[d, e], partner)
            copy.start()
            sends.append(copy)

        def arrive(e, d):
            piece(e, d, p_send.at[d - 1, e], p_recv.at[d - 1, e], plane[1]).wait_recv()

        def pass_on(e):
            a = 1 if e % 2 == 0 else 2
            b = 3 - a
            arrive(e, a)
            copy = piece(e, a, p_send.at[2, e], p_recv.at[2, e], plane[b])
            copy.start()
            sends.append(copy)
            hand(e, a)
            arrive(e, b)
            hand(e, b)

        spread(0)
        for e in range(1, line):
            piece(e, 0, z_send.at[e - 1], z_recv.at[e - 1], along[e]).wait_recv()
            spread(e)
            pass_on(e - 1)
        pass_on(line - 1)
        for e in range(line):
            arrive(e, 3)
            hand(e, 3)
        other = (1 - grp) * shards
        for e in range(line):
            for d in range(PLANE):
                place = full.at[other + behind[e] * PLANE + lows[d]]
                remote(place, place, g_send.at[d, e], g_recv.at[d, e], partner).wait_recv()
        for copy in sends:
            copy.wait_send()

    def rotation(norm_left):
        diag_bar, residual = bidiag[0], bidiag[1]
        radius = jnp.sqrt(diag_bar * diag_bar + norm_left * norm_left)
        cosine = diag_bar / radius
        sine = norm_left / radius
        return radius, cosine, sine, residual

    def advance(radius, cosine, residual):
        step = cosine * residual / radius
        for j in range(COLS_OWN):
            place = slice(j * 128, (j + 1) * 128)
            sol_ref[:, place] = sol_ref[:, place] + step * search[j]

    bidiag[0] = jnp.ones((8, 128), F32)
    bidiag[1] = jnp.zeros((8, 128), F32)

    def iterate(it, carry):
        lax.fori_loop(0, count // 4, adjoint, 0)
        summed = reduce_scatter()
        norm_left = jnp.sqrt(total(summed[HALF]))
        squares = jnp.zeros((8, 128), F32)
        mine = slot(0, 0)
        previous = own[pl.ds(grp * HALF, HALF)]
        fresh = summed[0:HALF] / norm_left[None] - norm_left[None] * previous
        full[mine, 0:HALF] = fresh
        full[mine, HALF] = jnp.sum(fresh * fresh, axis=0)
        all_gather()
        norm_right = jnp.sqrt(total(jnp.sum(full[:, HALF], axis=0)))
        radius, cosine, sine, residual = rotation(norm_left)
        advance(radius, cosine, residual)
        shrink = sine * norm_right / radius
        for half in range(2):
            fresh = full[half * shards + me, 0:HALF] / norm_right[None]
            own[half * HALF:(half + 1) * HALF] = fresh
            search[half * HALF:(half + 1) * HALF] = (
                fresh - shrink[None] * search[half * HALF:(half + 1) * HALF]
            )
        bidiag[0] = jnp.where(it == 0, norm_right, -cosine * norm_right)
        bidiag[1] = jnp.where(it == 0, norm_left, sine * residual)
        bidiag[2] = jnp.where(it == 0, norm_left, bidiag[2])
        lax.fori_loop(0, count // 4, forward, 0)
        out = jnp.dot(gather_rows[...], prod[...], preferred_element_type=F32)
        out = (out[:, 0:128] + out[:, 128:256]).reshape(rows, 8, 128)
        fresh = out / norm_right[None] - norm_right[None] * (left[...] / norm_left[None])
        left[...] = fresh
        norms[0] = jnp.sum(fresh * fresh, axis=0)
        return carry

    bidiag[2] = jnp.zeros((8, 128), F32)
    lax.fori_loop(0, ITERS, iterate, 0)

    sent = []
    for i, device in enumerate((partner, plane[1], plane[2])):
        copy = remote(norms.at[i], norms_in.at[i], n_send.at[i], n_recv.at[i], device)
        copy.start()
        copy.wait_recv()
        norms[i + 1] = norms[i] + norms_in[i]
        sent.append(copy)
    summed = norms[3]
    for e in range(1, line):
        copy = remote(
            norms.at[3], norms_in.at[2 + e], n_send.at[2 + e], n_recv.at[2 + e], along[e]
        )
        copy.start()
        sent.append(copy)
    for e in range(1, line):
        sent[2 + e].wait_recv()
        summed = summed + norms_in[2 + e]
    norm_left = jnp.sqrt(total(summed))
    radius, cosine, sine, residual = rotation(norm_left)
    advance(radius, cosine, residual)
    for r in range(rows):
        left_out[:, r * 128:(r + 1) * 128] = left[r] / norm_left
    rel_ref[...] = sine * residual / bidiag[2]
    for copy in sent:
        copy.wait_send()


def on_device(blocks, block_row, block_owner, block_col, right_side):
    count = blocks.shape[0]
    rows = right_side.shape[0] // 128
    shards = lax.axis_size("shard")
    line = shards // PLANE
    owner = block_owner[:, 0]
    place = ((block_col // HALF) * shards + owner) * HALF + block_col % HALF
    both = jnp.stack([place, block_row % rows])
    codes = (both[:, :, None] * 8 + jnp.arange(8, dtype=jnp.int32)).reshape(2, count * 8)
    piece = (HALF + 1, 8, 128)
    smem = pl.BlockSpec(memory_space=pltpu.SMEM)
    vmem = pl.BlockSpec(memory_space=pltpu.VMEM)
    dma = pltpu.SemaphoreType.DMA
    sol, left, rel = pl.pallas_call(
        functools.partial(kernel, shards, count, rows),
        out_shape=(
            jax.ShapeDtypeStruct((8, COLS_OWN * 128), F32),
            jax.ShapeDtypeStruct((8, rows * 128), F32),
            jax.ShapeDtypeStruct((8, 128), F32),
        ),
        in_specs=[smem, smem, smem, vmem, pl.BlockSpec(memory_space=pl.ANY), vmem],
        out_specs=(vmem, vmem, vmem),
        scratch_shapes=[
            pltpu.VMEM((count, 128, 128), F32),
            pltpu.VMEM((count, 128, 256), BF16),
            pltpu.VMEM((2 * shards, HALF * 8, count * 8), BF16),
            pltpu.VMEM((rows * 8, count * 8), BF16),
            pltpu.VMEM((count * 8, 256), BF16),
            pltpu.VMEM((rows, 8, 128), F32),
            pltpu.VMEM((8, 128), F32),
            pltpu.VMEM((8, 128), F32),
            pltpu.VMEM((2 * shards,) + piece, F32),
            pltpu.VMEM((2 * shards,) + piece, F32),
            pltpu.VMEM((shards,) + piece, F32),
            pltpu.VMEM((line, 2) + piece, F32),
            pltpu.VMEM((line,) + piece, F32),
            pltpu.VMEM((line,) + piece, F32),
            pltpu.VMEM((line - 1,) + piece, F32),
            pltpu.VMEM((line,) + piece, F32),
            pltpu.VMEM((4, 8, 128), F32),
            pltpu.VMEM((2 + line, 8, 128), F32),
            pltpu.VMEM((COLS_OWN, 8, 128), F32),
            pltpu.VMEM((COLS_OWN, 8, 128), F32),
            pltpu.VMEM((3, 8, 128), F32),
            dma((LOADS,)),
            dma((line,)), dma((line,)),
            dma((line, 2)), dma((line, 2)),
            dma((line,)), dma((line,)),
            dma((line - 1,)), dma((line - 1,)),
            dma((line - 1,)), dma((line - 1,)),
            dma((3, line)), dma((3, line)),
            dma((PLANE, line)), dma((PLANE, line)),
            dma((2 + line,)), dma((2 + line,)),
        ],
        compiler_params=pltpu.CompilerParams(
            collective_id=0, has_side_effects=True, vmem_limit_bytes=60 * 1024 * 1024
        ),
    )(owner, block_col, block_row, codes, blocks, right_side.T)
    return (sol.T, left.T, rel[:, 0])


def solution(mesh):
    placed = (
        P(("grp", "shard"), None, None),
        P(("grp", "shard")),
        P(("grp", "shard"), None),
        P(("grp", "shard")),
        P(("grp", "shard"), None),
    )
    return jax.shard_map(
        on_device,
        mesh=mesh,
        in_specs=placed,
        out_specs=(P("shard", None), P(("grp", "shard"), None), P()),
        check_vma=False,
    )
```

```python
import functools

import jax
import jax.numpy as jnp
from jax import lax
from jax.experimental import pallas as pl
from jax.experimental.pallas import tpu as pltpu
from jax.sharding import PartitionSpec as P

ITERS = 4
COLS_OWN = 16
HALF = COLS_OWN // 2
PLANE = 4
LOADS = 8
GROUP = 32
MESH = pl.DeviceIdType.MESH
F32 = jnp.float32
BF16 = jnp.bfloat16


def split(value):
    high = value.astype(BF16).astype(F32)
    return high, value - high


def total(tile):
    return jnp.broadcast_to(jnp.sum(tile, axis=-1, keepdims=True), tile.shape)


def kernel(
    shards, count, rows,
    owner_ref, col_ref, row_ref, code_ref, blocks_ref, right_ref,
    sol_ref, left_out, rel_ref,
    raw, pair, scatter, gather_rows, prod, left, unit, image,
    full, part, cross, from_a, from_z, to_z, norms, norms_in,
    own, search, bidiag,
    load_sem, x_send, x_recv, a_send, a_recv, c_send, c_recv,
    z_send, z_recv, p_send, p_recv, g_send, g_recv, n_send, n_recv,
):
    line = shards // PLANE
    grp = lax.axis_index("grp")
    me = lax.axis_index("shard")
    high, low = me // PLANE, me % PLANE

    def flip(index, d, size):
        out, weight = 0, 1
        while weight < size:
            bit = (index // weight) % 2
            if d & weight:
                bit = 1 - bit
            out = out + bit * weight
            weight *= 2
        return out

    lows = [flip(low, d, PLANE) for d in range(PLANE)]
    ahead = [flip(high, e, line) for e in range(line)]
    partner = (1 - grp, me)
    plane = {d: (grp, high * PLANE + lows[d]) for d in (1, 2, 3)}
    along = {e: (grp, ahead[e] * PLANE + low) for e in range(1, line)}

    def remote(src, dst, send, recv, device):
        return pltpu.make_async_remote_copy(
            src_ref=src, dst_ref=dst, send_sem=send, recv_sem=recv,
            device_id=device, device_id_type=MESH,
        )

    per_load = count // LOADS
    loads = [
        pltpu.make_async_copy(
            blocks_ref.at[pl.ds(i * per_load, per_load)],
            raw.at[pl.ds(i * per_load, per_load)],
            load_sem.at[i],
        )
        for i in range(LOADS)
    ]
    for copy in loads:
        copy.start()

    barrier = pltpu.get_barrier_semaphore()
    greeted = [partner, plane[1], plane[2], plane[3]] + [along[e] for e in range(1, line)]
    for device in greeted:
        pl.semaphore_signal(barrier, inc=1, device_id=device, device_id_type=MESH)

    squares = jnp.zeros((8, 128), F32)
    for r in range(rows):
        tile = right_ref[:, r * 128:(r + 1) * 128]
        left[r] = tile
        squares = squares + tile * tile
    norms[0] = squares

    codes = code_ref[0:1, :]
    row_codes = code_ref[1:2, :]
    ids = lax.broadcasted_iota(jnp.int32, (HALF * 8, count * 8), 0)

    def build(q, carry):
        scatter[q] = jnp.where(ids + q * (HALF * 8) == codes, 1.0, 0.0).astype(BF16)
        return carry

    lax.fori_loop(0, 2 * shards, build, 0)
    row_ids = lax.broadcasted_iota(jnp.int32, (rows * 8, count * 8), 0)
    gather_rows[...] = jnp.where(row_ids == row_codes, 1.0, 0.0).astype(BF16)

    for i, copy in enumerate(loads):
        copy.wait()

        def narrow(k, carry):
            block = raw[k]
            upper = block.astype(BF16)
            pair[k, :, 0:128] = upper
            pair[k, :, 128:256] = (block - upper.astype(F32)).astype(BF16)
            return carry

        lax.fori_loop(i * per_load, (i + 1) * per_load, narrow, 0, unroll=2)

    for j in range(COLS_OWN):
        own[j] = jnp.zeros((8, 128), F32)
        search[j] = jnp.zeros((8, 128), F32)
        sol_ref[:, j * 128:(j + 1) * 128] = jnp.zeros((8, 128), F32)

    pl.semaphore_wait(barrier, len(greeted))

    def both(tile):
        upper, lower = split(tile)
        return jnp.concatenate([upper, lower], axis=0).astype(BF16)

    def store_products(step, tiles):
        merged = jnp.concatenate(tiles, axis=0)
        upper, lower = split(merged)
        start = pl.multiple_of(step * 8 * len(tiles), 16)
        prod[pl.ds(start, 8 * len(tiles)), 0:128] = upper.astype(BF16)
        prod[pl.ds(start, 8 * len(tiles)), 128:256] = lower.astype(BF16)

    def adjoint(step, carry):
        tiles = []
        for i in range(GROUP):
            k = step * GROUP + i
            out = jnp.dot(both(left[row_ref[k] % rows]), pair[k], preferred_element_type=F32)
            out = out[:, 0:128] + out[:, 128:256]
            tiles.append(out[0:8] + out[8:16])
        store_products(step, tiles)
        return carry

    def forward(step, carry):
        tiles = []
        for i in range(GROUP):
            k = step * GROUP + i
            col = col_ref[k]
            tile = full[(col // HALF) * shards + owner_ref[k], col % HALF]
            lhs = both(tile)
            lhs = jnp.concatenate([lhs, lhs], axis=1)
            out = lax.dot_general(
                lhs, pair[k], (((1,), (1,)), ((), ())), preferred_element_type=F32
            )
            tiles.append(out[0:8] + out[8:16])
        store_products(step, tiles)
        return carry

    def columns_of(half):
        for c in range(shards // 16):
            base = half * shards + c * 16
            lhs = scatter[pl.ds(base, 16)].reshape(16 * HALF * 8, count * 8)
            out = jnp.dot(lhs, prod[...], preferred_element_type=F32)
            out = out[:, 0:128] + out[:, 128:256]
            part[pl.ds(base, 16), 0:HALF] = out.reshape(16, HALF, 8, 128)
            part[pl.ds(base, 16), HALF] = jnp.broadcast_to(norms[0][None], (16, 8, 128))

    def reduce_scatter():
        sends = []
        columns_of(1 - grp)
        order = list(range(line - 1, -1, -1))
        exchange = {}
        for e in order:
            first = ahead[e] * PLANE
            exchange[e] = remote(
                part.at[pl.ds((1 - grp) * shards + first, PLANE)],
                cross.at[pl.ds(first, PLANE)],
                x_send.at[e], x_recv.at[e], partner,
            )
            exchange[e].start()
        columns_of(grp)
        stage_a = {}
        for e in order:
            exchange[e].wait_recv()
            first = ahead[e] * PLANE
            cross[pl.ds(first, PLANE)] = (
                cross[pl.ds(first, PLANE)] + part[pl.ds(grp * shards + first, PLANE)]
            )
            for d in (1, 2, 3):
                copy = remote(
                    cross.at[first + lows[d]], from_a.at[e, d - 1],
                    a_send.at[e, d - 1], a_recv.at[e, d - 1], plane[d],
                )
                copy.start()
                stage_a[e, d] = copy
        stage_c = {}
        for e in order:
            mine = cross[ahead[e] * PLANE + low]
            for d in (1, 2, 3):
                stage_a[e, d].wait_recv()
                mine = mine + from_a[e, d - 1]
            to_z[e] = mine
            if e:
                stage_c[e] = remote(
                    to_z.at[e], from_z.at[e - 1], c_send.at[e - 1], c_recv.at[e - 1], along[e]
                )
                stage_c[e].start()
        for e in range(1, line):
            stage_c[e].wait_recv()
        summed = to_z[0]
        for e in range(1, line):
            summed = summed + from_z[e - 1]
        for copies in (exchange, stage_a, stage_c):
            for copy in copies.values():
                copy.wait_send()
        return summed

    def slot(e, d):
        return grp * shards + ahead[e] * PLANE + lows[d]

    def all_gather():
        sends = []

        def piece(e, d, send, recv, device):
            place = full.at[slot(e, d)]
            return remote(place, place, send, recv, device)

        for e in range(1, line):
            copy = piece(0, 0, z_send.at[e - 1], z_recv.at[e - 1], along[e])
            copy.start()
            sends.append(copy)

        def spread(e):
            for d in (1, 2, 3):
                copy = piece(e, 0, p_send.at[d - 1, e], p_recv.at[d - 1, e], plane[d])
                copy.start()
                sends.append(copy)
            hand(e, 0)

        def hand(e, d):
            copy = piece(e, d, g_send.at[d, e], g_recv.at[d, e], partner)
            copy.start()
            sends.append(copy)

        def arrive(e, d):
            piece(e, d, p_send.at[d - 1, e], p_recv.at[d - 1, e], plane[1]).wait_recv()

        spread(0)
        for e in range(1, line):
            piece(e, 0, z_send.at[e - 1], z_recv.at[e - 1], along[e]).wait_recv()
            spread(e)
        for e in range(line):
            for d in (1, 2, 3):
                arrive(e, d)
                hand(e, d)
        other = (1 - grp) * shards
        for e in range(line):
            for d in range(PLANE):
                place = full.at[other + ahead[e] * PLANE + lows[d]]
                remote(place, place, g_send.at[d, e], g_recv.at[d, e], partner).wait_recv()
        for copy in sends:
            copy.wait_send()

    def rotation(norm_left):
        diag_bar, residual = bidiag[0], bidiag[1]
        radius = jnp.sqrt(diag_bar * diag_bar + norm_left * norm_left)
        cosine = diag_bar / radius
        sine = norm_left / radius
        return radius, cosine, sine, residual

    def advance(radius, cosine, residual):
        step = cosine * residual / radius
        for j in range(COLS_OWN):
            place = slice(j * 128, (j + 1) * 128)
            sol_ref[:, place] = sol_ref[:, place] + step * search[j]

    bidiag[0] = jnp.ones((8, 128), F32)
    bidiag[1] = jnp.zeros((8, 128), F32)

    def iterate(it, carry):
        lax.fori_loop(0, count // GROUP, adjoint, 0)
        summed = reduce_scatter()
        norm_left = jnp.sqrt(total(summed[HALF]))
        squares = jnp.zeros((8, 128), F32)
        mine = slot(0, 0)
        previous = own[pl.ds(grp * HALF, HALF)]
        fresh = summed[0:HALF] / norm_left[None] - norm_left[None] * previous
        full[mine, 0:HALF] = fresh
        full[mine, HALF] = jnp.sum(fresh * fresh, axis=0)
        all_gather()
        norm_right = jnp.sqrt(total(jnp.sum(full[:, HALF], axis=0)))
        radius, cosine, sine, residual = rotation(norm_left)
        advance(radius, cosine, residual)
        shrink = sine * norm_right / radius
        for half in range(2):
            fresh = full[half * shards + me, 0:HALF] / norm_right[None]
            own[half * HALF:(half + 1) * HALF] = fresh
            search[half * HALF:(half + 1) * HALF] = (
                fresh - shrink[None] * search[half * HALF:(half + 1) * HALF]
            )
        bidiag[0] = jnp.where(it == 0, norm_right, -cosine * norm_right)
        bidiag[1] = jnp.where(it == 0, norm_left, sine * residual)
        bidiag[2] = jnp.where(it == 0, norm_left, bidiag[2])
        lax.fori_loop(0, count // GROUP, forward, 0)
        out = jnp.dot(gather_rows[...], prod[...], preferred_element_type=F32)
        out = (out[:, 0:128] + out[:, 128:256]).reshape(rows, 8, 128)
        fresh = out / norm_right[None] - norm_right[None] * (left[...] / norm_left[None])
        left[...] = fresh
        norms[0] = jnp.sum(fresh * fresh, axis=0)
        return carry

    bidiag[2] = jnp.zeros((8, 128), F32)
    lax.fori_loop(0, ITERS, iterate, 0)

    def swap(i, first, devices):
        copies = [
            remote(norms.at[i], norms_in.at[first + x], n_send.at[first + x], n_recv.at[first + x], y)
            for x, y in enumerate(devices)
        ]
        for copy in copies:
            copy.start()
        summed = norms[i]
        for x, copy in enumerate(copies):
            copy.wait_recv()
            summed = summed + norms_in[first + x]
        sent.extend(copies)
        return summed

    sent = []
    norms[1] = swap(0, 0, [partner])
    norms[2] = swap(1, 1, [plane[d] for d in (1, 2, 3)])
    summed = swap(2, 4, [along[e] for e in range(1, line)])
    norm_left = jnp.sqrt(total(summed))
    radius, cosine, sine, residual = rotation(norm_left)
    advance(radius, cosine, residual)
    for r in range(rows):
        left_out[:, r * 128:(r + 1) * 128] = left[r] / norm_left
    rel_ref[...] = sine * residual / bidiag[2]
    for copy in sent:
        copy.wait_send()


def on_device(blocks, block_row, block_owner, block_col, right_side):
    count = blocks.shape[0]
    rows = right_side.shape[0] // 128
    shards = lax.axis_size("shard")
    line = shards // PLANE
    owner = block_owner[:, 0]
    place = ((block_col // HALF) * shards + owner) * HALF + block_col % HALF
    both = jnp.stack([place, block_row % rows])
    codes = (both[:, :, None] * 8 + jnp.arange(8, dtype=jnp.int32)).reshape(2, count * 8)
    piece = (HALF + 1, 8, 128)
    smem = pl.BlockSpec(memory_space=pltpu.SMEM)
    vmem = pl.BlockSpec(memory_space=pltpu.VMEM)
    dma = pltpu.SemaphoreType.DMA
    sol, left, rel = pl.pallas_call(
        functools.partial(kernel, shards, count, rows),
        out_shape=(
            jax.ShapeDtypeStruct((8, COLS_OWN * 128), F32),
            jax.ShapeDtypeStruct((8, rows * 128), F32),
            jax.ShapeDtypeStruct((8, 128), F32),
        ),
        in_specs=[smem, smem, smem, vmem, pl.BlockSpec(memory_space=pl.ANY), vmem],
        out_specs=(vmem, vmem, vmem),
        scratch_shapes=[
            pltpu.VMEM((count, 128, 128), F32),
            pltpu.VMEM((count, 128, 256), BF16),
            pltpu.VMEM((2 * shards, HALF * 8, count * 8), BF16),
            pltpu.VMEM((rows * 8, count * 8), BF16),
            pltpu.VMEM((count * 8, 256), BF16),
            pltpu.VMEM((rows, 8, 128), F32),
            pltpu.VMEM((8, 128), F32),
            pltpu.VMEM((8, 128), F32),
            pltpu.VMEM((2 * shards,) + piece, F32),
            pltpu.VMEM((2 * shards,) + piece, F32),
            pltpu.VMEM((shards,) + piece, F32),
            pltpu.VMEM((line, 3) + piece, F32),
            pltpu.VMEM((line - 1,) + piece, F32),
            pltpu.VMEM((line,) + piece, F32),
            pltpu.VMEM((3, 8, 128), F32),
            pltpu.VMEM((3 + line, 8, 128), F32),
            pltpu.VMEM((COLS_OWN, 8, 128), F32),
            pltpu.VMEM((COLS_OWN, 8, 128), F32),
            pltpu.VMEM((3, 8, 128), F32),
            dma((LOADS,)),
            dma((line,)), dma((line,)),
            dma((line, 3)), dma((line, 3)),
            dma((line - 1,)), dma((line - 1,)),
            dma((line - 1,)), dma((line - 1,)),
            dma((3, line)), dma((3, line)),
            dma((PLANE, line)), dma((PLANE, line)),
            dma((3 + line,)), dma((3 + line,)),
        ],
        compiler_params=pltpu.CompilerParams(
            collective_id=0, has_side_effects=True, vmem_limit_bytes=60 * 1024 * 1024
        ),
    )(owner, block_col, block_row, codes, blocks, right_side.T)
    return (sol.T, left.T, rel[:, 0])


def solution(mesh):
    placed = (
        P(("grp", "shard"), None, None),
        P(("grp", "shard")),
        P(("grp", "shard"), None),
        P(("grp", "shard")),
        P(("grp", "shard"), None),
    )
    return jax.shard_map(
        on_device,
        mesh=mesh,
        in_specs=placed,
        out_specs=(P("shard", None), P(("grp", "shard"), None), P()),
        check_vma=False,
    )
```

```python
import functools

import jax
import jax.numpy as jnp
from jax import lax
from jax.experimental import pallas as pl
from jax.experimental.pallas import tpu as pltpu
from jax.sharding import PartitionSpec as P

ITERS = 4
COLS_OWN = 16
HALF = COLS_OWN // 2
PLANE = 4
LOADS = 8
GROUP = 32
MESH = pl.DeviceIdType.MESH
F32 = jnp.float32
BF16 = jnp.bfloat16


def split(value):
    high = value.astype(BF16).astype(F32)
    return high, value - high


def total(tile):
    return jnp.broadcast_to(jnp.sum(tile, axis=-1, keepdims=True), tile.shape)


def kernel(
    shards, count, rows,
    owner_ref, col_ref, row_ref, blocks_ref, right_ref,
    sol_ref, left_out, rel_ref,
    raw, pair, scatter, gather_rows, prod, left, unit, image,
    full, part, cross, from_a, from_z, to_z, norms, norms_in, partial,
    own, search, bidiag,
    load_sem, x_send, x_recv, a_send, a_recv, c_send, c_recv,
    z_send, z_recv, p_send, p_recv, g_send, g_recv, n_send, n_recv,
):
    line = shards // PLANE
    grp = lax.axis_index("grp")
    me = lax.axis_index("shard")
    high, low = me // PLANE, me % PLANE

    def flip(index, d, size):
        out, weight = 0, 1
        while weight < size:
            bit = (index // weight) % 2
            if d & weight:
                bit = 1 - bit
            out = out + bit * weight
            weight *= 2
        return out

    lows = [flip(low, d, PLANE) for d in range(PLANE)]
    ahead = [flip(high, e, line) for e in range(line)]
    partner = (1 - grp, me)
    plane = {d: (grp, high * PLANE + lows[d]) for d in (1, 2, 3)}
    along = {e: (grp, ahead[e] * PLANE + low) for e in range(1, line)}

    def remote(src, dst, send, recv, device):
        return pltpu.make_async_remote_copy(
            src_ref=src, dst_ref=dst, send_sem=send, recv_sem=recv,
            device_id=device, device_id_type=MESH,
        )

    per_load = count // LOADS
    loads = [
        pltpu.make_async_copy(
            blocks_ref.at[pl.ds(i * per_load, per_load)],
            raw.at[pl.ds(i * per_load, per_load)],
            load_sem.at[i],
        )
        for i in range(LOADS)
    ]
    for copy in loads:
        copy.start()

    barrier = pltpu.get_barrier_semaphore()
    greeted = [partner, plane[1], plane[2], plane[3]] + [along[e] for e in range(1, line)]
    for device in greeted:
        pl.semaphore_signal(barrier, inc=1, device_id=device, device_id_type=MESH)

    squares = jnp.zeros((8, 128), F32)
    for r in range(rows):
        tile = right_ref[:, r * 128:(r + 1) * 128]
        left[r] = tile
        squares = squares + tile * tile
    partial[...] = squares

    lanes = lax.broadcasted_iota(jnp.int32, (8, count * 8), 1)

    def code(k, carry):
        codes, row_codes = carry
        col = col_ref[k]
        place = ((col // HALF) * shards + owner_ref[k]) * HALF + col % HALF
        here = (lanes >= k * 8) & (lanes < k * 8 + 8)
        shift = lanes - k * 8
        return (
            jnp.where(here, place * 8 + shift, codes),
            jnp.where(here, (row_ref[k] % rows) * 8 + shift, row_codes),
        )

    codes, row_codes = lax.fori_loop(
        0, count, code, (jnp.zeros_like(lanes), jnp.zeros_like(lanes)), unroll=4
    )
    codes, row_codes = codes[0:1], row_codes[0:1]
    ids = lax.broadcasted_iota(jnp.int32, (HALF * 8, count * 8), 0)

    def build(q, carry):
        scatter[q] = jnp.where(ids + q * (HALF * 8) == codes, 1.0, 0.0).astype(BF16)
        return carry

    lax.fori_loop(0, 2 * shards, build, 0)
    row_ids = lax.broadcasted_iota(jnp.int32, (rows * 8, count * 8), 0)
    gather_rows[...] = jnp.where(row_ids == row_codes, 1.0, 0.0).astype(BF16)

    for i, copy in enumerate(loads):
        copy.wait()

        def narrow(k, carry):
            block = raw[k]
            upper = block.astype(BF16)
            pair[k, :, 0:128] = upper
            pair[k, :, 128:256] = (block - upper.astype(F32)).astype(BF16)
            return carry

        lax.fori_loop(i * per_load, (i + 1) * per_load, narrow, 0, unroll=2)

    for j in range(COLS_OWN):
        own[j] = jnp.zeros((8, 128), F32)
        search[j] = jnp.zeros((8, 128), F32)
        sol_ref[:, j * 128:(j + 1) * 128] = jnp.zeros((8, 128), F32)

    pl.semaphore_wait(barrier, len(greeted))

    def both(tile):
        upper, lower = split(tile)
        return jnp.concatenate([upper, lower], axis=0).astype(BF16)

    def store_products(step, tiles):
        merged = jnp.concatenate(tiles, axis=0)
        upper, lower = split(merged)
        start = pl.multiple_of(step * 8 * len(tiles), 16)
        prod[pl.ds(start, 8 * len(tiles)), 0:128] = upper.astype(BF16)
        prod[pl.ds(start, 8 * len(tiles)), 128:256] = lower.astype(BF16)

    def adjoint(step, carry):
        tiles = []
        for i in range(GROUP):
            k = step * GROUP + i
            out = jnp.dot(both(left[row_ref[k] % rows]), pair[k], preferred_element_type=F32)
            out = out[:, 0:128] + out[:, 128:256]
            tiles.append(out[0:8] + out[8:16])
        store_products(step, tiles)
        return carry

    def forward(step, carry):
        tiles = []
        for i in range(GROUP):
            k = step * GROUP + i
            col = col_ref[k]
            tile = full[(col // HALF) * shards + owner_ref[k], col % HALF]
            lhs = both(tile)
            lhs = jnp.concatenate([lhs, lhs], axis=1)
            out = lax.dot_general(
                lhs, pair[k], (((1,), (1,)), ((), ())), preferred_element_type=F32
            )
            tiles.append(out[0:8] + out[8:16])
        store_products(step, tiles)
        return carry

    def columns_of(half):
        for c in range(shards // 16):
            base = half * shards + c * 16
            lhs = scatter[pl.ds(base, 16)].reshape(16 * HALF * 8, count * 8)
            out = jnp.dot(lhs, prod[...], preferred_element_type=F32)
            out = out[:, 0:128] + out[:, 128:256]
            part[pl.ds(base, 16)] = out.reshape(16, HALF, 8, 128)

    def norm_exchange(kind, summed):
        sent = []
        first = 0
        hops = ([partner], [plane[d] for d in (1, 2, 3)], [along[e] for e in range(1, line)])
        for stage, devices in enumerate(hops):
            norms[kind, stage] = summed
            copies = []
            for x, device in enumerate(devices):
                at = first + x
                copies.append(remote(
                    norms.at[kind, stage], norms_in.at[kind, at],
                    n_send.at[kind, at], n_recv.at[kind, at], device,
                ))
                copies[-1].start()
            yield None
            for x, copy in enumerate(copies):
                copy.wait_recv()
                summed = summed + norms_in[kind, first + x]
            first += len(devices)
            sent += copies
        for copy in sent:
            copy.wait_send()
        yield summed

    def reduce_scatter(ends):
        next(ends)
        columns_of(1 - grp)
        order = list(range(line - 1, -1, -1))
        exchange = {}
        for e in order:
            first = ahead[e] * PLANE
            exchange[e] = remote(
                part.at[pl.ds((1 - grp) * shards + first, PLANE)],
                cross.at[pl.ds(first, PLANE)],
                x_send.at[e], x_recv.at[e], partner,
            )
            exchange[e].start()
        columns_of(grp)
        stage_a = {}
        for e in order:
            exchange[e].wait_recv()
            first = ahead[e] * PLANE
            cross[pl.ds(first, PLANE)] = (
                cross[pl.ds(first, PLANE)] + part[pl.ds(grp * shards + first, PLANE)]
            )
            for d in (1, 2, 3):
                copy = remote(
                    cross.at[first + lows[d]], from_a.at[e, d - 1],
                    a_send.at[e, d - 1], a_recv.at[e, d - 1], plane[d],
                )
                copy.start()
                stage_a[e, d] = copy
        next(ends)
        stage_c = {}
        for e in order:
            mine = cross[ahead[e] * PLANE + low]
            for d in (1, 2, 3):
                stage_a[e, d].wait_recv()
                mine = mine + from_a[e, d - 1]
            to_z[e] = mine
            if e:
                stage_c[e] = remote(
                    to_z.at[e], from_z.at[e - 1], c_send.at[e - 1], c_recv.at[e - 1], along[e]
                )
                stage_c[e].start()
        for e in range(1, line):
            stage_c[e].wait_recv()
        summed = to_z[0]
        for e in range(1, line):
            summed = summed + from_z[e - 1]
        for copies in (exchange, stage_a, stage_c):
            for copy in copies.values():
                copy.wait_send()
        return summed, next(ends)

    def slot(e, d):
        return grp * shards + ahead[e] * PLANE + lows[d]

    def all_gather(ends):
        next(ends)
        sends = []

        def piece(e, d, send, recv, device):
            place = full.at[slot(e, d)]
            return remote(place, place, send, recv, device)

        for e in range(1, line):
            copy = piece(0, 0, z_send.at[e - 1], z_recv.at[e - 1], along[e])
            copy.start()
            sends.append(copy)

        def spread(e):
            for d in (1, 2, 3):
                copy = piece(e, 0, p_send.at[d - 1, e], p_recv.at[d - 1, e], plane[d])
                copy.start()
                sends.append(copy)
            hand(e, 0)

        def hand(e, d):
            copy = piece(e, d, g_send.at[d, e], g_recv.at[d, e], partner)
            copy.start()
            sends.append(copy)

        def arrive(e, d):
            piece(e, d, p_send.at[d - 1, e], p_recv.at[d - 1, e], plane[1]).wait_recv()

        spread(0)
        for e in range(1, line):
            piece(e, 0, z_send.at[e - 1], z_recv.at[e - 1], along[e]).wait_recv()
            spread(e)
            if e == 1:
                next(ends)
        next(ends)
        for e in range(line):
            for d in (1, 2, 3):
                arrive(e, d)
                hand(e, d)
        other = (1 - grp) * shards
        for e in range(line):
            for d in range(PLANE):
                place = full.at[other + ahead[e] * PLANE + lows[d]]
                remote(place, place, g_send.at[d, e], g_recv.at[d, e], partner).wait_recv()
        for copy in sends:
            copy.wait_send()
        return next(ends)

    def rotation(norm_left):
        diag_bar, residual = bidiag[0], bidiag[1]
        radius = jnp.sqrt(diag_bar * diag_bar + norm_left * norm_left)
        cosine = diag_bar / radius
        sine = norm_left / radius
        return radius, cosine, sine, residual

    def advance(radius, cosine, residual):
        step = cosine * residual / radius
        for j in range(COLS_OWN):
            place = slice(j * 128, (j + 1) * 128)
            sol_ref[:, place] = sol_ref[:, place] + step * search[j]

    bidiag[0] = jnp.ones((8, 128), F32)
    bidiag[1] = jnp.zeros((8, 128), F32)

    def iterate(it, carry):
        ends = norm_exchange(0, partial[...])
        next(ends)
        lax.fori_loop(0, count // GROUP, adjoint, 0)
        summed, squares = reduce_scatter(ends)
        norm_left = jnp.sqrt(total(squares))
        mine = slot(0, 0)
        previous = own[pl.ds(grp * HALF, HALF)]
        fresh = summed / norm_left[None] - norm_left[None] * previous
        full[mine] = fresh
        squares = all_gather(norm_exchange(1, jnp.sum(fresh * fresh, axis=0)))
        norm_right = jnp.sqrt(total(squares))
        radius, cosine, sine, residual = rotation(norm_left)
        advance(radius, cosine, residual)
        shrink = sine * norm_right / radius
        for half in range(2):
            fresh = full[half * shards + me] / norm_right[None]
            own[half * HALF:(half + 1) * HALF] = fresh
            search[half * HALF:(half + 1) * HALF] = (
                fresh - shrink[None] * search[half * HALF:(half + 1) * HALF]
            )
        bidiag[0] = jnp.where(it == 0, norm_right, -cosine * norm_right)
        bidiag[1] = jnp.where(it == 0, norm_left, sine * residual)
        bidiag[2] = jnp.where(it == 0, norm_left, bidiag[2])
        lax.fori_loop(0, count // GROUP, forward, 0)
        out = jnp.dot(gather_rows[...], prod[...], preferred_element_type=F32)
        out = (out[:, 0:128] + out[:, 128:256]).reshape(rows, 8, 128)
        fresh = out / norm_right[None] - norm_right[None] * (left[...] / norm_left[None])
        left[...] = fresh
        partial[...] = jnp.sum(fresh * fresh, axis=0)
        return carry

    bidiag[2] = jnp.zeros((8, 128), F32)
    lax.fori_loop(0, ITERS, iterate, 0)

    ends = norm_exchange(0, partial[...])
    for _ in range(3):
        next(ends)
    summed = next(ends)
    norm_left = jnp.sqrt(total(summed))
    radius, cosine, sine, residual = rotation(norm_left)
    advance(radius, cosine, residual)
    for r in range(rows):
        left_out[:, r * 128:(r + 1) * 128] = left[r] / norm_left
    rel_ref[...] = sine * residual / bidiag[2]


def on_device(blocks, block_row, block_owner, block_col, right_side):
    count = blocks.shape[0]
    rows = right_side.shape[0] // 128
    shards = lax.axis_size("shard")
    line = shards // PLANE
    owner = block_owner[:, 0]
    piece = (HALF, 8, 128)
    smem = pl.BlockSpec(memory_space=pltpu.SMEM)
    vmem = pl.BlockSpec(memory_space=pltpu.VMEM)
    dma = pltpu.SemaphoreType.DMA
    sol, left, rel = pl.pallas_call(
        functools.partial(kernel, shards, count, rows),
        out_shape=(
            jax.ShapeDtypeStruct((8, COLS_OWN * 128), F32),
            jax.ShapeDtypeStruct((8, rows * 128), F32),
            jax.ShapeDtypeStruct((8, 128), F32),
        ),
        in_specs=[smem, smem, smem, pl.BlockSpec(memory_space=pl.ANY), vmem],
        out_specs=(vmem, vmem, vmem),
        scratch_shapes=[
            pltpu.VMEM((count, 128, 128), F32),
            pltpu.VMEM((count, 128, 256), BF16),
            pltpu.VMEM((2 * shards, HALF * 8, count * 8), BF16),
            pltpu.VMEM((rows * 8, count * 8), BF16),
            pltpu.VMEM((count * 8, 256), BF16),
            pltpu.VMEM((rows, 8, 128), F32),
            pltpu.VMEM((8, 128), F32),
            pltpu.VMEM((8, 128), F32),
            pltpu.VMEM((2 * shards,) + piece, F32),
            pltpu.VMEM((2 * shards,) + piece, F32),
            pltpu.VMEM((shards,) + piece, F32),
            pltpu.VMEM((line, 3) + piece, F32),
            pltpu.VMEM((line - 1,) + piece, F32),
            pltpu.VMEM((line,) + piece, F32),
            pltpu.VMEM((2, 3, 8, 128), F32),
            pltpu.VMEM((2, 3 + line, 8, 128), F32),
            pltpu.VMEM((8, 128), F32),
            pltpu.VMEM((COLS_OWN, 8, 128), F32),
            pltpu.VMEM((COLS_OWN, 8, 128), F32),
            pltpu.VMEM((3, 8, 128), F32),
            dma((LOADS,)),
            dma((line,)), dma((line,)),
            dma((line, 3)), dma((line, 3)),
            dma((line - 1,)), dma((line - 1,)),
            dma((line - 1,)), dma((line - 1,)),
            dma((3, line)), dma((3, line)),
            dma((PLANE, line)), dma((PLANE, line)),
            dma((2, 3 + line)), dma((2, 3 + line)),
        ],
        compiler_params=pltpu.CompilerParams(
            collective_id=0, has_side_effects=True, vmem_limit_bytes=60 * 1024 * 1024
        ),
    )(owner, block_col, block_row, blocks, right_side.T)
    return (sol.T, left.T, rel[:, 0])


def solution(mesh):
    placed = (
        P(("grp", "shard"), None, None),
        P(("grp", "shard")),
        P(("grp", "shard"), None),
        P(("grp", "shard")),
        P(("grp", "shard"), None),
    )
    return jax.shard_map(
        on_device,
        mesh=mesh,
        in_specs=placed,
        out_specs=(P("shard", None), P(("grp", "shard"), None), P()),
        check_vma=False,
    )
```

```python
import functools

import jax
import jax.numpy as jnp
from jax import lax
from jax.experimental import pallas as pl
from jax.experimental.pallas import tpu as pltpu
from jax.sharding import PartitionSpec as P

ITERS = 4
COLS_OWN = 16
HALF = COLS_OWN // 2
PLANE = 4
LOADS = 8
GROUP = 32
MESH = pl.DeviceIdType.MESH
F32 = jnp.float32
BF16 = jnp.bfloat16


def split(value):
    high = value.astype(BF16).astype(F32)
    return high, value - high


def total(tile):
    return jnp.broadcast_to(jnp.sum(tile, axis=-1, keepdims=True), tile.shape)


def kernel(
    shards, count, rows,
    owner_ref, col_ref, row_ref, blocks_ref, right_ref,
    sol_ref, left_out, rel_ref,
    raw, pair, scatter, gather_rows, prod, left, unit, image,
    full, part, cross, from_a, from_z, to_z, norms, norms_in, partial,
    own, search, bidiag,
    load_sem, x_send, x_recv, a_send, a_recv, c_send, c_recv,
    z_send, z_recv, p_send, p_recv, g_send, g_recv, n_send, n_recv,
):
    line = shards // PLANE
    grp = lax.axis_index("grp")
    me = lax.axis_index("shard")
    high, low = me // PLANE, me % PLANE

    def flip(index, d, size):
        out, weight = 0, 1
        while weight < size:
            bit = (index // weight) % 2
            if d & weight:
                bit = 1 - bit
            out = out + bit * weight
            weight *= 2
        return out

    lows = [flip(low, d, PLANE) for d in range(PLANE)]
    ahead = [flip(high, e, line) for e in range(line)]
    partner = (1 - grp, me)
    plane = {d: (grp, high * PLANE + lows[d]) for d in (1, 2, 3)}
    slant = [(1 - grp, high * PLANE + lows[d]) for d in (1, 2, 3)]
    along = {e: (grp, ahead[e] * PLANE + low) for e in range(1, line)}

    def remote(src, dst, send, recv, device):
        return pltpu.make_async_remote_copy(
            src_ref=src, dst_ref=dst, send_sem=send, recv_sem=recv,
            device_id=device, device_id_type=MESH,
        )

    per_load = count // LOADS
    loads = [
        pltpu.make_async_copy(
            blocks_ref.at[pl.ds(i * per_load, per_load)],
            raw.at[pl.ds(i * per_load, per_load)],
            load_sem.at[i],
        )
        for i in range(LOADS)
    ]
    for copy in loads:
        copy.start()

    barrier = pltpu.get_barrier_semaphore()
    greeted = [partner, plane[1], plane[2], plane[3]] + slant + [along[e] for e in range(1, line)]
    for device in greeted:
        pl.semaphore_signal(barrier, inc=1, device_id=device, device_id_type=MESH)

    squares = jnp.zeros((8, 128), F32)
    for r in range(rows):
        tile = right_ref[:, r * 128:(r + 1) * 128]
        left[r] = tile
        squares = squares + tile * tile
    partial[...] = squares

    lanes = lax.broadcasted_iota(jnp.int32, (8, count * 8), 1)

    def code(k, carry):
        codes, row_codes = carry
        col = col_ref[k]
        place = ((col // HALF) * shards + owner_ref[k]) * HALF + col % HALF
        here = (lanes >= k * 8) & (lanes < k * 8 + 8)
        shift = lanes - k * 8
        return (
            jnp.where(here, place * 8 + shift, codes),
            jnp.where(here, (row_ref[k] % rows) * 8 + shift, row_codes),
        )

    codes, row_codes = lax.fori_loop(
        0, count, code, (jnp.zeros_like(lanes), jnp.zeros_like(lanes)), unroll=4
    )
    codes, row_codes = codes[0:1], row_codes[0:1]
    ids = lax.broadcasted_iota(jnp.int32, (HALF * 8, count * 8), 0)

    def build(q, carry):
        scatter[q] = jnp.where(ids + q * (HALF * 8) == codes, 1.0, 0.0).astype(BF16)
        return carry

    lax.fori_loop(0, 2 * shards, build, 0)
    row_ids = lax.broadcasted_iota(jnp.int32, (rows * 8, count * 8), 0)
    gather_rows[...] = jnp.where(row_ids == row_codes, 1.0, 0.0).astype(BF16)

    for i, copy in enumerate(loads):
        copy.wait()

        def narrow(k, carry):
            block = raw[k]
            upper = block.astype(BF16)
            pair[k, :, 0:128] = upper
            pair[k, :, 128:256] = (block - upper.astype(F32)).astype(BF16)
            return carry

        lax.fori_loop(i * per_load, (i + 1) * per_load, narrow, 0, unroll=2)

    for j in range(COLS_OWN):
        own[j] = jnp.zeros((8, 128), F32)
        search[j] = jnp.zeros((8, 128), F32)
        sol_ref[:, j * 128:(j + 1) * 128] = jnp.zeros((8, 128), F32)

    pl.semaphore_wait(barrier, len(greeted))

    def both(tile):
        upper, lower = split(tile)
        return jnp.concatenate([upper, lower], axis=0).astype(BF16)

    def store_products(step, tiles):
        merged = jnp.concatenate(tiles, axis=0)
        upper, lower = split(merged)
        start = pl.multiple_of(step * 8 * len(tiles), 16)
        prod[pl.ds(start, 8 * len(tiles)), 0:128] = upper.astype(BF16)
        prod[pl.ds(start, 8 * len(tiles)), 128:256] = lower.astype(BF16)

    def adjoint(step, carry):
        tiles = []
        for i in range(GROUP):
            k = step * GROUP + i
            out = jnp.dot(both(left[row_ref[k] % rows]), pair[k], preferred_element_type=F32)
            out = out[:, 0:128] + out[:, 128:256]
            tiles.append(out[0:8] + out[8:16])
        store_products(step, tiles)
        return carry

    def forward(step, carry):
        tiles = []
        for i in range(GROUP):
            k = step * GROUP + i
            col = col_ref[k]
            tile = full[(col // HALF) * shards + owner_ref[k], col % HALF]
            lhs = both(tile)
            lhs = jnp.concatenate([lhs, lhs], axis=1)
            out = lax.dot_general(
                lhs, pair[k], (((1,), (1,)), ((), ())), preferred_element_type=F32
            )
            tiles.append(out[0:8] + out[8:16])
        store_products(step, tiles)
        return carry

    def columns_of(half):
        for c in range(shards // 16):
            base = half * shards + c * 16
            lhs = scatter[pl.ds(base, 16)].reshape(16 * HALF * 8, count * 8)
            out = jnp.dot(lhs, prod[...], preferred_element_type=F32)
            out = out[:, 0:128] + out[:, 128:256]
            part[pl.ds(base, 16)] = out.reshape(16, HALF, 8, 128)

    def norm_exchange(kind, summed):
        sent = []
        first = 0
        hops = (
            [partner] + [plane[d] for d in (1, 2, 3)] + slant,
            [along[e] for e in range(1, line)],
        )
        for stage, devices in enumerate(hops):
            norms[kind, stage] = summed
            copies = []
            for x, device in enumerate(devices):
                at = first + x
                copies.append(remote(
                    norms.at[kind, stage], norms_in.at[kind, at],
                    n_send.at[kind, at], n_recv.at[kind, at], device,
                ))
                copies[-1].start()
            yield None
            for x, copy in enumerate(copies):
                copy.wait_recv()
                summed = summed + norms_in[kind, first + x]
            first += len(devices)
            sent += copies
        for copy in sent:
            copy.wait_send()
        yield summed

    def reduce_scatter(ends):
        columns_of(1 - grp)
        order = list(range(line - 1, -1, -1))
        exchange = {}
        for e in order:
            first = ahead[e] * PLANE
            exchange[e] = remote(
                part.at[pl.ds((1 - grp) * shards + first, PLANE)],
                cross.at[pl.ds(first, PLANE)],
                x_send.at[e], x_recv.at[e], partner,
            )
            exchange[e].start()
        columns_of(grp)
        stage_a = {}
        for e in order:
            exchange[e].wait_recv()
            first = ahead[e] * PLANE
            cross[pl.ds(first, PLANE)] = (
                cross[pl.ds(first, PLANE)] + part[pl.ds(grp * shards + first, PLANE)]
            )
            for d in (1, 2, 3):
                copy = remote(
                    cross.at[first + lows[d]], from_a.at[e, d - 1],
                    a_send.at[e, d - 1], a_recv.at[e, d - 1], plane[d],
                )
                copy.start()
                stage_a[e, d] = copy
        next(ends)
        stage_c = {}
        for e in order:
            mine = cross[ahead[e] * PLANE + low]
            for d in (1, 2, 3):
                stage_a[e, d].wait_recv()
                mine = mine + from_a[e, d - 1]
            to_z[e] = mine
            if e:
                stage_c[e] = remote(
                    to_z.at[e], from_z.at[e - 1], c_send.at[e - 1], c_recv.at[e - 1], along[e]
                )
                stage_c[e].start()
        for e in range(1, line):
            stage_c[e].wait_recv()
        summed = to_z[0]
        for e in range(1, line):
            summed = summed + from_z[e - 1]
        for copies in (exchange, stage_a, stage_c):
            for copy in copies.values():
                copy.wait_send()
        return summed, next(ends)

    def slot(e, d):
        return grp * shards + ahead[e] * PLANE + lows[d]

    def all_gather(ends):
        next(ends)
        sends = []

        def piece(e, d, send, recv, device):
            place = full.at[slot(e, d)]
            return remote(place, place, send, recv, device)

        for e in range(1, line):
            copy = piece(0, 0, z_send.at[e - 1], z_recv.at[e - 1], along[e])
            copy.start()
            sends.append(copy)

        def spread(e):
            for d in (1, 2, 3):
                copy = piece(e, 0, p_send.at[d - 1, e], p_recv.at[d - 1, e], plane[d])
                copy.start()
                sends.append(copy)
            hand(e, 0)

        def hand(e, d):
            copy = piece(e, d, g_send.at[d, e], g_recv.at[d, e], partner)
            copy.start()
            sends.append(copy)

        def arrive(e, d):
            piece(e, d, p_send.at[d - 1, e], p_recv.at[d - 1, e], plane[1]).wait_recv()

        spread(0)
        for e in range(1, line):
            piece(e, 0, z_send.at[e - 1], z_recv.at[e - 1], along[e]).wait_recv()
            spread(e)
            if e == 1:
                next(ends)
        for e in range(line):
            for d in (1, 2, 3):
                arrive(e, d)
                hand(e, d)
        other = (1 - grp) * shards
        for e in range(line):
            for d in range(PLANE):
                place = full.at[other + ahead[e] * PLANE + lows[d]]
                remote(place, place, g_send.at[d, e], g_recv.at[d, e], partner).wait_recv()
        for copy in sends:
            copy.wait_send()
        return next(ends)

    def rotation(norm_left):
        diag_bar, residual = bidiag[0], bidiag[1]
        radius = jnp.sqrt(diag_bar * diag_bar + norm_left * norm_left)
        cosine = diag_bar / radius
        sine = norm_left / radius
        return radius, cosine, sine, residual

    def advance(radius, cosine, residual):
        step = cosine * residual / radius
        for j in range(COLS_OWN):
            place = slice(j * 128, (j + 1) * 128)
            sol_ref[:, place] = sol_ref[:, place] + step * search[j]

    bidiag[0] = jnp.ones((8, 128), F32)
    bidiag[1] = jnp.zeros((8, 128), F32)

    def iterate(it, carry):
        ends = norm_exchange(0, partial[...])
        next(ends)
        lax.fori_loop(0, count // GROUP, adjoint, 0)
        summed, squares = reduce_scatter(ends)
        norm_left = jnp.sqrt(total(squares))
        mine = slot(0, 0)
        previous = own[pl.ds(grp * HALF, HALF)]
        fresh = summed / norm_left[None] - norm_left[None] * previous
        full[mine] = fresh
        squares = all_gather(norm_exchange(1, jnp.sum(fresh * fresh, axis=0)))
        norm_right = jnp.sqrt(total(squares))
        radius, cosine, sine, residual = rotation(norm_left)
        advance(radius, cosine, residual)
        shrink = sine * norm_right / radius
        for half in range(2):
            fresh = full[half * shards + me] / norm_right[None]
            own[half * HALF:(half + 1) * HALF] = fresh
            search[half * HALF:(half + 1) * HALF] = (
                fresh - shrink[None] * search[half * HALF:(half + 1) * HALF]
            )
        bidiag[0] = jnp.where(it == 0, norm_right, -cosine * norm_right)
        bidiag[1] = jnp.where(it == 0, norm_left, sine * residual)
        bidiag[2] = jnp.where(it == 0, norm_left, bidiag[2])
        lax.fori_loop(0, count // GROUP, forward, 0)
        out = jnp.dot(gather_rows[...], prod[...], preferred_element_type=F32)
        out = (out[:, 0:128] + out[:, 128:256]).reshape(rows, 8, 128)
        fresh = out / norm_right[None] - norm_right[None] * (left[...] / norm_left[None])
        left[...] = fresh
        partial[...] = jnp.sum(fresh * fresh, axis=0)
        return carry

    bidiag[2] = jnp.zeros((8, 128), F32)
    lax.fori_loop(0, ITERS, iterate, 0)

    ends = norm_exchange(0, partial[...])
    for _ in range(2):
        next(ends)
    summed = next(ends)
    norm_left = jnp.sqrt(total(summed))
    radius, cosine, sine, residual = rotation(norm_left)
    advance(radius, cosine, residual)
    for r in range(rows):
        left_out[:, r * 128:(r + 1) * 128] = left[r] / norm_left
    rel_ref[...] = sine * residual / bidiag[2]


def on_device(blocks, block_row, block_owner, block_col, right_side):
    count = blocks.shape[0]
    rows = right_side.shape[0] // 128
    shards = lax.axis_size("shard")
    line = shards // PLANE
    owner = block_owner[:, 0]
    piece = (HALF, 8, 128)
    smem = pl.BlockSpec(memory_space=pltpu.SMEM)
    vmem = pl.BlockSpec(memory_space=pltpu.VMEM)
    dma = pltpu.SemaphoreType.DMA
    sol, left, rel = pl.pallas_call(
        functools.partial(kernel, shards, count, rows),
        out_shape=(
            jax.ShapeDtypeStruct((8, COLS_OWN * 128), F32),
            jax.ShapeDtypeStruct((8, rows * 128), F32),
            jax.ShapeDtypeStruct((8, 128), F32),
        ),
        in_specs=[smem, smem, smem, pl.BlockSpec(memory_space=pl.ANY), vmem],
        out_specs=(vmem, vmem, vmem),
        scratch_shapes=[
            pltpu.VMEM((count, 128, 128), F32),
            pltpu.VMEM((count, 128, 256), BF16),
            pltpu.VMEM((2 * shards, HALF * 8, count * 8), BF16),
            pltpu.VMEM((rows * 8, count * 8), BF16),
            pltpu.VMEM((count * 8, 256), BF16),
            pltpu.VMEM((rows, 8, 128), F32),
            pltpu.VMEM((8, 128), F32),
            pltpu.VMEM((8, 128), F32),
            pltpu.VMEM((2 * shards,) + piece, F32),
            pltpu.VMEM((2 * shards,) + piece, F32),
            pltpu.VMEM((shards,) + piece, F32),
            pltpu.VMEM((line, 3) + piece, F32),
            pltpu.VMEM((line - 1,) + piece, F32),
            pltpu.VMEM((line,) + piece, F32),
            pltpu.VMEM((2, 2, 8, 128), F32),
            pltpu.VMEM((2, 6 + line, 8, 128), F32),
            pltpu.VMEM((8, 128), F32),
            pltpu.VMEM((COLS_OWN, 8, 128), F32),
            pltpu.VMEM((COLS_OWN, 8, 128), F32),
            pltpu.VMEM((3, 8, 128), F32),
            dma((LOADS,)),
            dma((line,)), dma((line,)),
            dma((line, 3)), dma((line, 3)),
            dma((line - 1,)), dma((line - 1,)),
            dma((line - 1,)), dma((line - 1,)),
            dma((3, line)), dma((3, line)),
            dma((PLANE, line)), dma((PLANE, line)),
            dma((2, 6 + line)), dma((2, 6 + line)),
        ],
        compiler_params=pltpu.CompilerParams(
            collective_id=0, has_side_effects=True, vmem_limit_bytes=60 * 1024 * 1024
        ),
    )(owner, block_col, block_row, blocks, right_side.T)
    return (sol.T, left.T, rel[:, 0])


def solution(mesh):
    placed = (
        P(("grp", "shard"), None, None),
        P(("grp", "shard")),
        P(("grp", "shard"), None),
        P(("grp", "shard")),
        P(("grp", "shard"), None),
    )
    return jax.shard_map(
        on_device,
        mesh=mesh,
        in_specs=placed,
        out_specs=(P("shard", None), P(("grp", "shard"), None), P()),
        check_vma=False,
    )
```
